32 devices in a mesh: rep: 4 (over y, x), wide: 8 (over z, core).
Axes of the slice: x: 2, y: 2, z: 4, core: 2. Of those that a mesh axis runs over, the one named last changes fastest.
Arguments:
- hot_table: bfloat16 [16384, 128], P('wide'), may hold values from -3 to 3
- cold_table: bfloat16 [65536, 128], P(('rep', 'wide')), may hold values from -3 to 3
- bag_of: int32 [32, 6144], P(('rep', 'wide')), may hold values from 0 to 4095, never falling along the last dimension, each value on 1 to 4 neighbouring positions
- owner: int32 [196608, 1], P(('rep', 'wide')), may hold values from 0 to 39; in each aligned block of 6144 rows (0 to 6143, 6144 to 12287, ...) at most 232 rows name the same one
- row_in: int32 [196608], P(('rep', 'wide')), may hold values from 0 to 2047
- cross_down: bfloat16 [4096, 256], replicated, may hold values from -0.09375 to 0.09375
- cross_up: bfloat16 [4096, 256], replicated, may hold values from -0.375 to 0.375
- cross_bias: float32 [4096], replicated, may hold values from -3 to 3
- top_weight: bfloat16 [4096, 512], replicated, may hold values from -0.09375 to 0.09375
- d_hidden: bfloat16 [4096, 512], P(('rep', 'wide')), may hold values from -6 to 6
Outputs:
- grad_up: float32 [4096, 256], P(('rep', 'wide'))
- grad_down: float32 [4096, 256], P(('rep', 'wide'))
- grad_top: float32 [4096, 512], P(('rep', 'wide'))
- hot_grad: float32 [16384, 128], P('wide')
- cold_grad: float32 [65536, 128], P(('rep', 'wide'))
The draws below stay inside these ranges and needn't reach their ends.
Inputs may be any that keep to these rules, and one draw needn't show every extreme that they name: Destination of each lookup: below 8 the holder of hot rows at that wide index in the asking device's own rep group, else the holder of cold rows numbered owner minus 8 over rep+wide. Among the 6144 lookups of one device no destination is named more than 232 times, and in every draw some device names some destination exactly 232 times. `bag_of`: never falls along one device's lookups; each of a device's 4096 bags has 1 to 4 lookups, and some bag has 4. Bag b is sample b // 32, feature b % 32 of the device.
All inputs are finite; a program needn't handle non-finite values.
Results may differ from the reference program's by a relative error of at most 0.0064.
Values may be sent and summed in bfloat16 or wider, within the bound.
No kernel may reach another device: no remote copies, remote signals or barrier semaphores. Data moves between devices by JAX's collectives and lax.ppermute only.
A program may use at most 128 MiB of HBM per device.

```python
import math
import jax
import jax.numpy as jnp
import numpy as np
from jax import lax

E = 128
R = 256
H = 512
MOST = 4
B_DEV = 128
ROWS_DEV = 2048
D = 4096
BAGS_DEV = 4096
LOOK_DEV = 6144
SHARDS = 32
DESTS = 40
CAP = 232
BATCH = 4096
LOOKUPS = 196608
HOT = 16384
COLD = 65536
N_WIDE = 8


def set_ends(values, key, least, top_value):
    longest = values.shape.index(max(values.shape))
    spots = []
    for shift in (0, 1):
        where = [jax.random.randint(jax.random.fold_in(key, axis), (), 0, length) for axis, length in enumerate(values.shape)]
        where[longest] = (where[longest] + shift) % values.shape[longest]
        spots.append(tuple(where))
    return values.at[spots[0]].set(least).at[spots[1]].set(top_value)


def block_scale(key, shape, cuts, low, top_value):
    level, own = 1.0, jax.random.fold_in(key, 6)
    for axis_at, shards_of in cuts:
        steps = jnp.exp(jax.random.uniform(jax.random.fold_in(own, axis_at), (shards_of,), jnp.float32, low / len(cuts), top_value / len(cuts)))
        level = level * jnp.repeat(steps, shape[axis_at] // shards_of).reshape([-1 if axis == axis_at else 1 for axis in range(len(shape))])
    return level


def profile(amount, total, limit, slope):
    portions = [(1 << 20) // math.isqrt(rank ** slope) + 1 for rank in range(2, amount + 1)]
    rest, counts = total - limit - (amount - 1), [1] * (amount - 1)
    while rest > 0:
        free = [i for i in range(amount - 1) if counts[i] < limit]
        whole, budget = sum([portions[i] for i in free]), rest
        for i in free:
            addition = min(limit - counts[i], max(1, budget * portions[i] // whole), rest)
            counts[i] = counts[i] + addition
            rest = rest - addition
    return np.array([limit] + counts)


def ragged_sizes(stream_key, count, total, most, skew):
    if count == 2:
        one = jax.random.randint(stream_key, (), max(1, total - most), min(most, total - 1) + 1)
        return jnp.stack([one, total - one])
    tallies = jnp.asarray(profile(count, total, most, skew), jnp.int32)
    pairs = (count - 1) // 2
    giver, taker = tallies[1:1 + 2 * pairs:2], tallies[2:2 + 2 * pairs:2]
    room = jnp.minimum(giver - 1, most - taker)
    shifted = jax.random.randint(jax.random.fold_in(stream_key, 1), (pairs,), 0, 1 << 20) % (room + 1)
    tallies = tallies.at[1:1 + 2 * pairs:2].set(giver - shifted).at[2:2 + 2 * pairs:2].set(taker + shifted)
    return tallies[jax.random.permutation(jax.random.fold_in(stream_key, 2), count)]


def routed_block(own_key, own, number, rows, amount, top, reach, slope):
    ranking = jax.random.permutation(own_key, amount)
    heavy_load, ordinary = shares(amount, rows * top, reach, slope, True), shares(amount, rows * top, reach, slope, False)
    places = jnp.arange(amount)

    def named(lengths, offset_by):
        used = int((lengths > 0).sum())
        fixed = max(1, used // 4)
        shifted = fixed + (places - fixed + offset_by * (used - fixed)) % max(1, amount - fixed)
        return jnp.zeros((amount,), jnp.int32).at[ranking[jnp.where(places < fixed, places, shifted)]].set(jnp.asarray(lengths, jnp.int32))

    lengths = jnp.where(number % 4 == 0, named(heavy_load, number // 4), named(ordinary, number - number // 4 - 1))
    mixed = jax.random.permutation(jax.random.fold_in(own, 3), amount)
    donor, taker = mixed[0:amount // 2 * 2:2], mixed[1:amount // 2 * 2:2]
    slack = jnp.minimum(lengths[donor] - 1, reach - lengths[taker]) // 2
    slack = jnp.where((donor == ranking[0]) | (taker == ranking[0]) | (lengths[taker] == 0), 0, jnp.maximum(slack, 0))
    shifted = jax.random.randint(jax.random.fold_in(own, 4), (amount // 2,), 0, 1 << 20) % (slack + 1)
    lengths = lengths.at[donor].add(-shifted).at[taker].add(shifted)
    labels = jnp.searchsorted(jnp.cumsum(lengths), jnp.arange(rows * top), side="right").astype(jnp.int32)
    grid = labels.reshape(top, rows).T
    grid = grid[jax.random.permutation(jax.random.fold_in(own, 1), rows)]
    offset_by = jax.random.randint(jax.random.fold_in(own, 2), (rows, 1), 0, top)
    return jnp.take_along_axis(grid, (jnp.arange(top)[None, :] + offset_by) % top, axis=1)


def shares(count, total, bound, skew, full):
    weights = [(1 << 20) // math.isqrt(grade ** skew) + 1 for grade in range(1, count + 1)]
    largest = bound if full else min(bound, max(-(-total // count), total * weights[0] // sum(weights)))
    least = 1 if total - largest >= count - 1 else 0
    given, rest = [largest] + [least] * (count - 1), total - largest - least * (count - 1)
    while rest > 0:
        free = [i for i in range(1, count) if given[i] < largest] or [i for i in range(1, count) if given[i] < bound]
        mass, budget = sum([weights[i] for i in free]), rest
        for i in free:
            extra = min(bound - given[i], max(1, budget * weights[i] // mass), rest)
            given[i] = given[i] + extra
            rest = rest - extra
    return np.array(given)


def gaussian(rng, dims, width, bound, shards=(), kind=jnp.bfloat16):
    loudness = block_scale(rng, dims, shards, -0.22, 0.18) if shards else 1.0
    entries = jax.random.normal(rng, dims, jnp.float32) * width * loudness
    return jnp.minimum(jnp.maximum(entries, -bound), bound).astype(kind)


def setup_inputs(seed: int = 0) -> dict:
    arg_keys = jax.random.split(jax.random.key(seed), 11)
    hot_table = gaussian(arg_keys[0], (HOT, E), 0.5, 3.0, ((0, 8),))
    cold_table = gaussian(arg_keys[1], (COLD, E), 0.5, 3.0, ((0, 32),))
    bag_of = jax.vmap(lambda own: jnp.searchsorted(jnp.cumsum(ragged_sizes(own, BAGS_DEV, LOOK_DEV, MOST, 2)), jnp.arange(LOOK_DEV), side="right"))(jax.random.split(arg_keys[2], SHARDS)).reshape((SHARDS, LOOK_DEV)).astype(jnp.int32)
    owner_keys = jax.random.split(jax.random.fold_in(arg_keys[3], 1), LOOKUPS // LOOK_DEV)
    owner_turns = jax.random.permutation(jax.random.fold_in(arg_keys[3], 3), LOOKUPS // LOOK_DEV)
    owner = jax.vmap(lambda own, number: routed_block(jax.random.fold_in(arg_keys[3], 2), own, number, LOOK_DEV, DESTS, 1, CAP, 2))(owner_keys, owner_turns).reshape((LOOKUPS, 1))
    row_in = set_ends(jax.random.randint(arg_keys[4], (LOOKUPS,), 0, ROWS_DEV), jax.random.fold_in(arg_keys[4], 1), 0, ROWS_DEV - 1).astype(jnp.int32)
    cross_down = gaussian(arg_keys[5], (D, R), D ** -0.5, 0.09375)
    cross_up = gaussian(arg_keys[6], (D, R), R ** -0.5, 0.375)
    cross_bias = gaussian(arg_keys[7], (D,), 0.5, 3.0, (), jnp.float32)
    top_weight = gaussian(arg_keys[8], (D, H), D ** -0.5, 0.09375)
    d_hidden = gaussian(arg_keys[9], (BATCH, H), 1.0, 6.0, ((0, 32),))
    return dict(hot_table=hot_table, cold_table=cold_table, bag_of=bag_of, owner=owner, row_in=row_in, cross_down=cross_down, cross_up=cross_up, cross_bias=cross_bias, top_weight=top_weight, d_hidden=d_hidden)


def dense_pass(base, grad_hidden, cross_down, cross_up, cross_bias, top_weight):
    low = jnp.dot(base, cross_down, preferred_element_type=jnp.float32).astype(jnp.bfloat16)
    cross = lax.dot_general(low, cross_up, (((1,), (1,)), ((), ())), preferred_element_type=jnp.float32) + cross_bias
    base_full = base.astype(jnp.float32)
    mixed = (base_full * cross + base_full).astype(jnp.bfloat16)
    preact = jnp.dot(mixed, top_weight, preferred_element_type=jnp.float32)
    sigm = jax.nn.sigmoid(preact)
    d_pre = (grad_hidden.astype(jnp.float32) * sigm * (1.0 + preact * (1.0 - sigm))).astype(jnp.bfloat16)
    d_mixed = lax.dot_general(d_pre, top_weight, (((1,), (1,)), ((), ())), preferred_element_type=jnp.float32)
    d_cross = (d_mixed * base_full).astype(jnp.bfloat16)
    d_low = jnp.dot(d_cross, cross_up, preferred_element_type=jnp.float32).astype(jnp.bfloat16)
    d_base = (d_mixed * (cross + 1.0) + lax.dot_general(d_low, cross_down, (((1,), (1,)), ((), ())), preferred_element_type=jnp.float32)).astype(jnp.bfloat16)
    contract = (((0,), (0,)), ((), ()))
    t_up = lax.dot_general(d_cross, low, contract, preferred_element_type=jnp.float32)
    t_down = lax.dot_general(base, d_low, contract, preferred_element_type=jnp.float32)
    t_top = lax.dot_general(mixed, d_pre, contract, preferred_element_type=jnp.float32)
    return (jnp.concatenate([t_up, t_down, t_top], axis=1), d_base)

def reference(hot_table, cold_table, bag_of, owner, row_in, cross_down, cross_up, cross_bias, top_weight, d_hidden):
    scale_factor = 1.0 / math.sqrt(BATCH)
    owners = owner.reshape(SHARDS, LOOK_DEV)
    rows_all = row_in.reshape(SHARDS, LOOK_DEV)
    grads_all = d_hidden.reshape(SHARDS, B_DEV, H)

    def device_step(carry, inputs):
        dense_sum, hot_sum, cold_sum = carry
        dest_list, row_list, bag_list, grad_hidden = inputs
        is_hot = dest_list < N_WIDE
        hot_index = jnp.where(is_hot, dest_list * ROWS_DEV + row_list, 0).astype(jnp.int32)
        cold_index = jnp.where(is_hot, 0, (dest_list - N_WIDE) * ROWS_DEV + row_list).astype(jnp.int32)
        values = jnp.where(is_hot[:, None], hot_table[hot_index], cold_table[cold_index])
        pooled = jax.ops.segment_sum(values.astype(jnp.float32), bag_list, num_segments=BAGS_DEV)
        base = pooled.reshape(B_DEV, D).astype(jnp.bfloat16)
        terms, d_base = dense_pass(base, grad_hidden, cross_down, cross_up, cross_bias, top_weight)
        per_look = d_base.reshape(BAGS_DEV, E)[bag_list].astype(jnp.float32)
        hot_target = jnp.where(is_hot, hot_index, HOT).astype(jnp.int32)
        cold_target = jnp.where(is_hot, COLD, cold_index).astype(jnp.int32)
        hot_sum = hot_sum.at[hot_target].add(per_look, mode='drop')
        cold_sum = cold_sum.at[cold_target].add(per_look, mode='drop')
        dense_sum = dense_sum + terms * scale_factor
        return ((dense_sum, hot_sum, cold_sum), None)
    start_carry = (jnp.zeros((D, 2 * R + H), jnp.float32), jnp.zeros((HOT, E), jnp.float32), jnp.zeros((COLD, E), jnp.float32))
    final_carry, unused = lax.scan(device_step, start_carry, (owners, rows_all, bag_of, grads_all))
    dense_sum, hot_sum, cold_sum = final_carry
    return (dense_sum[:, :R], dense_sum[:, R:2 * R], dense_sum[:, 2 * R:], hot_sum, cold_sum)
```

```python
import functools
import math

import jax
import jax.numpy as jnp
from jax import lax
from jax.experimental import pallas as pl
from jax.experimental.pallas import tpu as pltpu
from jax.sharding import Mesh
from jax.sharding import PartitionSpec as P

LANES = 128
CORES = 2
BF = jnp.bfloat16
F32 = jnp.float32
NT = (((1,), (1,)), ((), ()))


def round_up(value, unit):
    return (value + unit - 1) // unit * unit


def route_kernel(
    owner_ref, row_ref, bag_ref, slots_ref, rows_ref, bags_ref, carry, acc, *, n_rep, n_wide, cap, per_dest, hot_at
):
    blocks = owner_ref.shape[0]
    dests = carry.shape[0]
    shards, lanes = rows_ref.shape
    owner_ids = lax.broadcasted_iota(jnp.int32, (dests, LANES), 0)
    dest_ids = lax.broadcasted_iota(jnp.int32, (shards, LANES), 0)
    place_ids = lax.broadcasted_iota(jnp.int32, (lanes, LANES), 0)
    before = lax.broadcasted_iota(jnp.int32, (LANES, 2 * LANES), 0)
    after = lax.broadcasted_iota(jnp.int32, (LANES, 2 * LANES), 1)
    upper = jnp.where((before < after), 1.0, 0.0).astype(BF)
    carry[...] = jnp.zeros_like(carry)
    acc[...] = jnp.zeros_like(acc)

    def step(block, unused):
        own = owner_ref[pl.ds(block, 1), :]
        mine = owner_ids == own
        counts = jnp.dot(jnp.where(mine, 1.0, 0.0).astype(BF), upper, preferred_element_type=F32)
        earlier = counts[:, :LANES] + carry[...]
        carry[...] += counts[:, LANES:]
        rank = jnp.sum(jnp.where(mine, earlier, 0.0), axis=0, keepdims=True)
        layer = jnp.floor((rank + 0.5) * (1.0 / n_rep))
        copy_at = (rank - layer * n_rep).astype(jnp.int32)
        layer = layer.astype(jnp.int32)
        rank = rank.astype(jnp.int32)
        is_hot = own < n_wide
        dest = jnp.where(is_hot, copy_at * n_wide + own, own - n_wide)
        place = jnp.where(is_hot, hot_at + layer, rank)
        slots_ref[pl.ds(block, 1), :] = dest * per_dest + jnp.where(is_hot, cap + layer, rank)
        at_dest = dest_ids == dest
        at_place = jnp.where(place_ids == place, 1.0, 0.0).astype(BF)
        row = row_ref[pl.ds(block, 1), :] + 1
        bag = bag_ref[pl.ds(block, 1), :]
        planes = [row // 256, row % 256, bag // 256, bag % 256]
        left = jnp.concatenate([jnp.where(at_dest, plane.astype(F32), 0.0) for plane in planes], axis=0)
        acc[...] += lax.dot_general(left.astype(BF), at_place, NT, preferred_element_type=F32)
        return unused

    lax.fori_loop(0, blocks, step, 0)
    rows_ref[...] = (acc[:shards] * 256.0 + acc[shards : 2 * shards]).astype(jnp.int32)
    bags_ref[...] = (acc[2 * shards : 3 * shards] * 256.0 + acc[3 * shards :]).astype(jnp.int32)


def narrow(source, target):
    total = target.shape[0]
    step = math.gcd(total, 512)

    def move(at, unused):
        rows = pl.ds(pl.multiple_of(at * step, step), step)
        target[rows, :] = source[rows, :].astype(target.dtype)
        return unused

    lax.fori_loop(0, total // step, move, 0)


def widen(source, target):
    total = source.shape[0]
    step = math.gcd(total, 512)

    def move(at, unused):
        rows = pl.ds(pl.multiple_of(at * step, step), step)
        target[rows, :] = source[rows, :].astype(F32)
        return unused

    lax.fori_loop(0, total // step, move, 0)


def serve_kernel(ask_ref, cold_ref, hot_ref, out_ref, cold, hot, stage, *, cap, hot_cap, hot_at):
    shards = ask_ref.shape[0]
    per_dest = cap + hot_cap
    cold[0:8, :] = jnp.zeros((8, LANES), F32)
    hot[0:8, :] = jnp.zeros((8, LANES), F32)
    rows = cold_ref.shape[0]
    cold[8 : 8 + rows, :] = cold_ref[...].astype(F32)
    hot[8 : 8 + rows, :] = hot_ref[...].astype(F32)

    def step(source, unused):
        first = pl.multiple_of(source * per_dest, 8)
        for at in range(cap):
            stage[pl.ds(first + at, 1), :] = cold[pl.ds(ask_ref[source, at] + 7, 1), :]
        for at in range(hot_cap):
            stage[pl.ds(first + cap + at, 1), :] = hot[pl.ds(ask_ref[source, hot_at + at] + 7, 1), :]
        return unused

    lax.fori_loop(0, shards, step, 0)
    narrow(stage, out_ref)


def pool_kernel(slot_ref, first_ref, bag_ref, back_ref, base_ref, wide_rows, stage, pooled, *, features):
    blocks = slot_ref.shape[0]
    window = LANES + 8
    widen(back_ref, wide_rows)
    pooled[...] = jnp.zeros_like(pooled)
    places = lax.broadcasted_iota(jnp.int32, (window, LANES), 0)

    def step(block, unused):
        for at in range(LANES):
            stage[at : at + 1, :] = wide_rows[pl.ds(slot_ref[block, at], 1), :]
        start = pl.multiple_of(first_ref[block, 0] // 8 * 8, 8)
        member = jnp.where(places + start == bag_ref[pl.ds(block, 1), :], 1.0, 0.0).astype(BF)
        part = jnp.dot(member, stage[...].astype(BF), preferred_element_type=F32)
        pooled[pl.ds(start, window), :] += part
        return unused

    lax.fori_loop(0, blocks, step, 0)
    samples = base_ref.shape[0]
    for feature in range(features):
        base_ref[:, feature * LANES : (feature + 1) * LANES] = pooled[
            pl.ds(feature, samples, stride=features), :
        ].astype(BF)


def spread_kernel(bag_ref, grad_ref, out_ref, bag_rows, stage, *, cap, hot_cap, hot_at, features):
    shards = bag_ref.shape[0]
    per_dest = cap + hot_cap
    samples = grad_ref.shape[0]
    for feature in range(features):
        bag_rows[pl.ds(feature, samples, stride=features), :] = grad_ref[
            :, feature * LANES : (feature + 1) * LANES
        ].astype(F32)

    def step(dest, unused):
        first = pl.multiple_of(dest * per_dest, 8)
        for at in range(per_dest):
            place = at if at < cap else hot_at + at - cap
            stage[pl.ds(first + at, 1), :] = bag_rows[pl.ds(bag_ref[dest, place], 1), :]
        return unused

    lax.fori_loop(0, shards, step, 0)
    narrow(stage, out_ref)


def hot_sum_kernel(ask_ref, in_ref, out_ref, wide_rows, stage, acc, *, cap, hot_cap):
    blocks, span = ask_ref.shape
    per_dest = cap + hot_cap
    group = span // hot_cap
    rows = acc.shape[0]
    row_ids = lax.broadcasted_iota(jnp.int32, (rows, span), 0) + 1
    widen(in_ref, wide_rows)
    acc[...] = jnp.zeros_like(acc)

    def step(block, unused):
        for member in range(group):
            first = pl.multiple_of((block * group + member) * per_dest + cap, 8)
            stage[member * hot_cap : (member + 1) * hot_cap, :] = wide_rows[pl.ds(first, hot_cap), :]
        pick = jnp.where(row_ids == ask_ref[pl.ds(block, 1), :], 1.0, 0.0).astype(BF)
        acc[...] += jnp.dot(pick, stage[...].astype(BF), preferred_element_type=F32)
        return unused

    lax.fori_loop(0, blocks, step, 0)
    out_ref[...] = acc[...].astype(out_ref.dtype)


def cold_sum_kernel(ask_ref, in_ref, out_ref, wide_rows, *, cap, hot_cap, hot_at):
    shards = ask_ref.shape[0]
    per_dest = cap + hot_cap
    rows = out_ref.shape[0]
    total = in_ref.shape[0]
    row_ids = lax.broadcasted_iota(jnp.int32, (rows, hot_at), 0) + 1
    widen(in_ref, wide_rows)
    wide_rows[total:, :] = jnp.zeros((wide_rows.shape[0] - total, LANES), F32)
    out_ref[...] = jnp.zeros_like(out_ref)

    def step(source, unused):
        first = pl.multiple_of(source * per_dest, 8)
        pick = jnp.where(row_ids == ask_ref[pl.ds(source, 1), :][:, :hot_at], 1.0, 0.0).astype(BF)
        block = wide_rows[pl.ds(first, hot_at), :].astype(BF)
        out_ref[...] += jnp.dot(pick, block, preferred_element_type=F32)
        return unused

    lax.fori_loop(0, shards, step, 0)


def shaped(shape, dtype):
    return jax.ShapeDtypeStruct(shape, dtype)


SMEM = pl.BlockSpec(memory_space=pltpu.SMEM)
VMEM = pl.BlockSpec(memory_space=pltpu.VMEM)


def body(
    hot_table,
    cold_table,
    bag_of,
    owner,
    row_in,
    cross_down,
    cross_up,
    cross_bias,
    top_weight,
    d_hidden,
    interpret=False,
):
    n_rep = lax.axis_size("rep")
    n_line = lax.axis_size("line")
    n_wide = n_line * CORES
    shards = n_rep * n_wide
    dests = n_wide + shards
    look_dev = row_in.shape[0]
    rows_dev = hot_table.shape[0]
    width = hot_table.shape[1]
    batch_dev = d_hidden.shape[0]
    feat_width = cross_down.shape[0]
    rank_width = cross_down.shape[1]
    features = feat_width // width
    bags_dev = batch_dev * features
    cap = max(8, (3 * look_dev // (2 * dests) + 7) // 8 * 8)
    hot_cap = round_up(-(-cap // n_rep), 8)
    per_dest = cap + hot_cap
    hot_at = round_up(cap, LANES)
    lanes = hot_at + round_up(hot_cap, LANES)
    total = shards * per_dest
    blocks = look_dev // LANES
    everyone = ("rep", "line", "core")
    plane = ("rep", "core")

    owner_2d = owner.reshape(blocks, LANES)
    bag_2d = bag_of.reshape(blocks, LANES)
    slots, ask, bag_pick = pl.pallas_call(
        functools.partial(
            route_kernel, n_rep=n_rep, n_wide=n_wide, cap=cap, per_dest=per_dest, hot_at=hot_at
        ),
        out_shape=(
            shaped((blocks, LANES), jnp.int32),
            shaped((shards, lanes), jnp.int32),
            shaped((shards, lanes), jnp.int32),
        ),
        in_specs=[VMEM] * 3,
        out_specs=(VMEM,) * 3,
        scratch_shapes=[
            pltpu.VMEM((round_up(dests, 16), LANES), F32),
            pltpu.VMEM((4 * shards, lanes), F32),
        ],
        interpret=interpret,
        name="route",
    )(owner_2d, row_in.reshape(blocks, LANES), bag_2d)
    asked = lax.all_to_all(ask, everyone, split_axis=0, concat_axis=0, tiled=True)
    found = pl.pallas_call(
        functools.partial(serve_kernel, cap=cap, hot_cap=hot_cap, hot_at=hot_at),
        out_shape=shaped((total, width), BF),
        in_specs=[SMEM, VMEM, VMEM],
        out_specs=VMEM,
        scratch_shapes=[
            pltpu.VMEM((rows_dev + 8, width), F32),
            pltpu.VMEM((rows_dev + 8, width), F32),
            pltpu.VMEM((total, width), F32),
        ],
        interpret=interpret,
        name="serve",
    )(asked, cold_table, hot_table)
    back = lax.all_to_all(found, everyone, split_axis=0, concat_axis=0, tiled=True)
    base = pl.pallas_call(
        functools.partial(pool_kernel, features=features),
        out_shape=shaped((batch_dev, feat_width), BF),
        in_specs=[SMEM, SMEM, VMEM, VMEM],
        out_specs=VMEM,
        scratch_shapes=[
            pltpu.VMEM((total, width), F32),
            pltpu.VMEM((LANES, width), F32),
            pltpu.VMEM((bags_dev + LANES + 8, width), F32),
        ],
        interpret=interpret,
        name="pool",
    )(slots, bag_2d, bag_2d, back)

    def by_plane(value):
        parts = value.reshape(batch_dev, n_rep, n_line, CORES, feat_width // shards)
        return parts.transpose(1, 3, 0, 2, 4).reshape(n_rep * CORES, batch_dev, -1)

    def to_all(value):
        return jnp.broadcast_to(value[None], (n_rep * CORES,) + value.shape)

    def exchange(pieces):
        joined = jnp.concatenate(pieces, axis=2)
        moved = lax.all_to_all(joined, plane, split_axis=0, concat_axis=0, tiled=True)
        return moved.reshape(n_rep * CORES * batch_dev, -1)

    part_width = n_line * (feat_width // shards)
    low = jnp.dot(base, cross_down, preferred_element_type=F32).astype(BF)
    cross = lax.dot_general(low, cross_up, NT, preferred_element_type=F32) + cross_bias
    base_full = base.astype(F32)
    mixed = (base_full * cross + base_full).astype(BF)
    early = exchange([by_plane(base), by_plane(mixed), to_all(low)])
    preact = jnp.dot(mixed, top_weight, preferred_element_type=F32)
    sigm = jax.nn.sigmoid(preact)
    d_pre = (d_hidden.astype(F32) * sigm * (1.0 + preact * (1.0 - sigm))).astype(BF)
    d_mixed = lax.dot_general(d_pre, top_weight, NT, preferred_element_type=F32)
    d_cross = (d_mixed * base_full).astype(BF)
    d_low = jnp.dot(d_cross, cross_up, preferred_element_type=F32).astype(BF)
    d_base = (
        d_mixed * (cross + 1.0) + lax.dot_general(d_low, cross_down, NT, preferred_element_type=F32)
    ).astype(BF)
    outgoing = pl.pallas_call(
        functools.partial(
            spread_kernel, cap=cap, hot_cap=hot_cap, hot_at=hot_at, features=features
        ),
        out_shape=shaped((total, width), BF),
        in_specs=[SMEM, VMEM],
        out_specs=VMEM,
        scratch_shapes=[
            pltpu.VMEM((bags_dev, width), F32),
            pltpu.VMEM((total, width), F32),
        ],
        interpret=interpret,
        name="spread",
    )(bag_pick, d_base)
    incoming = lax.all_to_all(outgoing, everyone, split_axis=0, concat_axis=0, tiled=True)
    late = exchange([by_plane(d_cross), to_all(d_low), to_all(d_pre)])

    contract = (((0,), (0,)), ((), ()))
    all_base = early[:, :part_width]
    all_mixed = early[:, part_width : 2 * part_width]
    all_low = early[:, 2 * part_width :]
    all_cross = late[:, :part_width]
    all_d_low = late[:, part_width : part_width + rank_width]
    all_pre = late[:, part_width + rank_width :]
    t_up = lax.dot_general(all_cross, all_low, contract, preferred_element_type=F32)
    t_down = lax.dot_general(all_base, all_d_low, contract, preferred_element_type=F32)
    t_top = lax.dot_general(all_mixed, all_pre, contract, preferred_element_type=F32)
    part = jnp.concatenate([t_up, t_down, t_top], axis=1).astype(BF)
    part = lax.all_to_all(
        part.reshape(n_line, feat_width // shards, -1), "line", split_axis=0, concat_axis=0, tiled=True
    )
    scale_factor = 1.0 / math.sqrt(batch_dev * shards)
    summed = jnp.sum(part.astype(F32), axis=0) * scale_factor

    hot_span = math.gcd(shards * hot_cap, 256)
    hot_asked = asked[:, hot_at : hot_at + hot_cap].reshape(-1, hot_span)
    hot_part = pl.pallas_call(
        functools.partial(hot_sum_kernel, cap=cap, hot_cap=hot_cap),
        out_shape=shaped((rows_dev, width), BF),
        in_specs=[VMEM, VMEM],
        out_specs=VMEM,
        scratch_shapes=[
            pltpu.VMEM((total, width), F32),
            pltpu.VMEM((hot_span, width), F32),
            pltpu.VMEM((rows_dev, width), F32),
        ],
        interpret=interpret,
        name="hot_sum",
    )(hot_asked, incoming)
    hot_all = lax.all_to_all(
        jnp.broadcast_to(hot_part[None], (n_rep,) + hot_part.shape),
        "rep",
        split_axis=0,
        concat_axis=0,
        tiled=True,
    )
    hot_grad = jnp.sum(hot_all.astype(F32), axis=0)
    cold_grad = pl.pallas_call(
        functools.partial(cold_sum_kernel, cap=cap, hot_cap=hot_cap, hot_at=hot_at),
        out_shape=shaped((rows_dev, width), F32),
        in_specs=[VMEM, VMEM],
        out_specs=VMEM,
        scratch_shapes=[pltpu.VMEM((total + hot_at, width), F32)],
        interpret=interpret,
        name="cold_sum",
    )(asked, incoming)
    return (
        summed[:, :rank_width],
        summed[:, rank_width : 2 * rank_width],
        summed[:, 2 * rank_width :],
        hot_grad,
        cold_grad,
    )


def solution(mesh):
    n_rep, n_wide = mesh.devices.shape
    fine = Mesh(mesh.devices.reshape(n_rep, n_wide // CORES, CORES), ("rep", "line", "core"))
    every = ("rep", "line", "core")
    wide = ("line", "core")
    placed = (
        P(wide, None),
        P(every, None),
        P(every, None),
        P(every, None),
        P(every),
        P(),
        P(),
        P(),
        P(),
        P(every, None),
    )
    return jax.shard_map(
        body,
        mesh=fine,
        in_specs=placed,
        out_specs=(
            P(every, None),
            P(every, None),
            P(every, None),
            P(wide, None),
            P(every, None),
        ),
        check_vma=False,
    )
```
